256 devices in a mesh: ctx: 16 (over z, core), grp: 16 (over x, y).
Axes of the slice: x: 4, y: 4, z: 8, core: 2. Of those that a mesh axis runs over, the one named last changes fastest.
Arguments:
- queries: bfloat16 [4096, 8192], P('ctx', 'grp'), may hold values from -27 to 27, as said below
- keys: bfloat16 [4096, 1024], P('ctx'), may hold values from -27 to 27
- values: bfloat16 [4096, 1024], P('ctx'), may hold values from -6 to 6
- out_weight: bfloat16 [8192, 8192], P('grp'), may hold values from -0.0625 to 0.0625
- span_order: int32 [32], replicated, may hold values from 0 to 31, each once
- document: int32 [4096], replicated, may hold values from 0 to 3, never falling along the last dimension, each value on 1 to 2048 neighbouring positions
Outputs:
- projected: bfloat16 [4096, 8192], P('ctx', 'grp')
The draws below stay inside these ranges and needn't reach their ends.
Inputs may be any that keep to these rules, and one draw needn't show every extreme that they name: `queries`: queries and keys are of order one, except a few rows that may be larger.
All inputs are finite; a program needn't handle non-finite values.
Results may differ from the reference program's by a relative error of at most 0.023.
Values may be sent and summed in bfloat16 or wider, within the bound.
No kernel may reach another device: no remote copies, remote signals or barrier semaphores. Data moves between devices by JAX's collectives and lax.ppermute only.
A program may use at most 128 MiB of HBM per device.

```python
import math
import jax
import jax.numpy as jnp
import numpy as np
from jax import lax

MODEL_DIM = 8192
Q_HEADS = 64
KV_HEADS = 8
HEAD_DIM = 128
QUERY_GROUP = 8
SPAN = 128
SEQ = 4096
N_CTX = 16
N_GRP = 16


def drawn_fields(key):
    base_query = jnp.clip(jax.random.normal(jax.random.fold_in(key, 11), (SEQ, Q_HEADS * HEAD_DIM), jnp.float32), -5.0, 5.0)
    base_key = jnp.clip(jax.random.normal(jax.random.fold_in(key, 12), (SEQ, KV_HEADS * HEAD_DIM), jnp.float32), -5.0, 5.0)
    return (base_query, base_key)


def draw_queries(key, part):
    return drawn_fields(key)[0].astype(jnp.bfloat16)


def draw_keys(key, part):
    return drawn_fields(key)[1].astype(jnp.bfloat16)


def block_scale(rng, dims, shards, low, top_value):
    factor_of, own = 1.0, jax.random.fold_in(rng, 6)
    for axis_at, blocks in shards:
        heights = jnp.exp(jax.random.uniform(jax.random.fold_in(own, axis_at), (blocks,), jnp.float32, low / len(shards), top_value / len(shards)))
        factor_of = factor_of * jnp.repeat(heights, dims[axis_at] // blocks).reshape([-1 if axis == axis_at else 1 for axis in range(len(dims))])
    return factor_of


def split_up(count, total, limit, skew):
    loads = [(1 << 20) // math.isqrt(rank ** skew) + 1 for rank in range(2, count + 1)]
    rest, counts = total - limit - (count - 1), [1] * (count - 1)
    while rest > 0:
        movable = [i for i in range(count - 1) if counts[i] < limit]
        mass, budget = sum([loads[i] for i in movable]), rest
        for i in movable:
            more = min(limit - counts[i], max(1, budget * loads[i] // mass), rest)
            counts[i] = counts[i] + more
            rest = rest - more
    return np.array([limit] + counts)


def ragged_sizes(own_key, number_of, total, reach, lean):
    if number_of == 2:
        one = jax.random.randint(own_key, (), max(1, total - reach), min(reach, total - 1) + 1)
        return jnp.stack([one, total - one])
    sizes = jnp.asarray(split_up(number_of, total, reach, lean), jnp.int32)
    twos = (number_of - 1) // 2
    donor, sink = sizes[1:1 + 2 * twos:2], sizes[2:2 + 2 * twos:2]
    slack = jnp.minimum(donor - 1, reach - sink)
    passed = jax.random.randint(jax.random.fold_in(own_key, 1), (twos,), 0, 1 << 20) % (slack + 1)
    sizes = sizes.at[1:1 + 2 * twos:2].set(donor - passed).at[2:2 + 2 * twos:2].set(sink + passed)
    return sizes[jax.random.permutation(jax.random.fold_in(own_key, 2), number_of)]


def bell_draw(own_key, dims, deviation, limit, cuts=(), kind=jnp.bfloat16):
    entries = deviation * jax.random.normal(own_key, dims, jnp.float32)
    if cuts:
        entries = entries * block_scale(own_key, dims, cuts, -0.22, 0.18)
    return jnp.clip(entries, -limit, limit).astype(kind)


def setup_inputs(seed: int = 0) -> dict:
    seeds = jax.random.split(jax.random.key(seed), 7)
    queries = draw_queries(jax.random.fold_in(seeds[6], 71), 0)
    keys = draw_keys(jax.random.fold_in(seeds[6], 71), 0)
    values = bell_draw(seeds[2], (SEQ, KV_HEADS * HEAD_DIM), 1.0, 6.0, ((0, 16),))
    out_weight = bell_draw(seeds[3], (Q_HEADS * HEAD_DIM, MODEL_DIM), (Q_HEADS * HEAD_DIM) ** -0.5, 0.0625, ((0, 16),))
    span_order = jax.random.permutation(seeds[4], 2 * N_CTX).astype(jnp.int32)
    document = jnp.searchsorted(jnp.cumsum(ragged_sizes(seeds[5], 4, SEQ, SEQ // 2, 0)), jnp.arange(SEQ), side="right").astype(jnp.int32)
    return dict(queries=queries, keys=keys, values=values, out_weight=out_weight, span_order=span_order, document=document)


def row_positions(span_order):
    rows = jnp.arange(SEQ, dtype=jnp.int32)
    return (span_order[rows // SPAN] * SPAN + rows % SPAN).astype(jnp.int32)

def reference(queries, keys, values, out_weight, span_order, document):
    positions = row_positions(span_order)
    docs = document[positions]
    visible = (positions[None, :] <= positions[:, None]) & (docs[None, :] == docs[:, None])
    score_scale = 1.0 / math.sqrt(HEAD_DIM)

    def one_head(head):
        shared = head // QUERY_GROUP
        query_head = lax.dynamic_slice_in_dim(queries, head * HEAD_DIM, HEAD_DIM, 1)
        key_head = lax.dynamic_slice_in_dim(keys, shared * HEAD_DIM, HEAD_DIM, 1)
        value_head = lax.dynamic_slice_in_dim(values, shared * HEAD_DIM, HEAD_DIM, 1)
        scores = jnp.dot(query_head, key_head.T, preferred_element_type=jnp.float32) * score_scale
        scores = jnp.where(visible, scores, -jnp.inf)
        highest = lax.optimization_barrier(jnp.max(scores, axis=1, keepdims=True))
        probs = jnp.exp(scores - highest)
        total = lax.optimization_barrier(jnp.sum(probs, axis=1, keepdims=True))
        mixed = jnp.dot(probs.astype(jnp.bfloat16), value_head, preferred_element_type=jnp.float32)
        return (mixed / total).astype(jnp.bfloat16)
    attended = lax.map(one_head, jnp.arange(Q_HEADS, dtype=jnp.int32))
    block_heads = Q_HEADS // N_GRP

    def add_block(running, block):
        head_rows = lax.dynamic_slice_in_dim(attended, block * block_heads, block_heads, 0)
        weight_rows = lax.dynamic_slice_in_dim(out_weight, block * block_heads * HEAD_DIM, block_heads * HEAD_DIM, 0)
        weight_rows = weight_rows.reshape(block_heads, HEAD_DIM, MODEL_DIM)
        block_sum = jnp.einsum('hsd,hdm->sm', head_rows.astype(jnp.float32), weight_rows.astype(jnp.float32))
        rounded = lax.optimization_barrier(block_sum.astype(jnp.bfloat16))
        return (running + rounded.astype(jnp.float32), None)
    start = jnp.zeros((SEQ, MODEL_DIM), jnp.float32)
    projected, unused = lax.scan(add_block, start, jnp.arange(N_GRP, dtype=jnp.int32))
    return projected.astype(jnp.bfloat16)
```

```python
import math

import jax
import jax.numpy as jnp
from jax import lax
from jax.experimental import pallas as pl
from jax.experimental.pallas import tpu as pltpu
from jax.sharding import PartitionSpec as P

HEAD_DIM = 128
QUERY_GROUP = 8
SPAN = 128
CHUNK = 256
NEG = -1e30
NZ, NX, NY = 8, 4, 4

VMEM = pl.BlockSpec(memory_space=pltpu.VMEM)
SMEM = pl.BlockSpec(memory_space=pltpu.SMEM)


def along_z(k):
    return [(z * 2 + c, (z + k) % NZ * 2 + c) for z in range(NZ) for c in range(2)]


def along_x(k):
    return [(x * NY + y, (x + k) % NX * NY + y) for x in range(NX) for y in range(NY)]


def along_y(k):
    return [(x * NY + y, x * NY + (y + k) % NY) for x in range(NX) for y in range(NY)]


OTHER_CORE = [(i, i ^ 1) for i in range(2 * NZ)]


def gathered(own):
    blocks = {(0, 0): own}
    blocks[4, 0] = lax.ppermute(own, "ctx", along_z(-4))
    up = down = own
    for step in (1, 2, 3):
        down = lax.ppermute(down, "ctx", along_z(1))
        up = lax.ppermute(up, "ctx", along_z(-1))
        blocks[-step, 0], blocks[step, 0] = down, up
    for dz, dc in list(blocks):
        blocks[dz, 1] = lax.ppermute(blocks[dz, dc], "ctx", OTHER_CORE)
    return [(dz, dc, block) for (dz, dc), block in blocks.items()]


def attend_kernel(where, spans, doc_ref, q_ref, *refs):
    kv_refs, (out_ref, keys, values, acc) = refs[:-4], refs[-4:]
    ctx = where[0]
    zed, core = ctx // 2, ctx % 2
    for (dz, dc), kv in zip(ORDER, kv_refs):
        source = (zed + dz + NZ) % NZ * 2 + (core + dc) % 2
        for half in range(2):
            at = pl.multiple_of(spans[source * 2 + half] * SPAN, SPAN)
            rows = slice(half * SPAN, half * SPAN + SPAN)
            keys[pl.ds(at, SPAN), :] = kv[rows, :HEAD_DIM]
            values[pl.ds(at, SPAN), :] = kv[rows, HEAD_DIM:]

    docs = doc_ref[...]
    starts = [jnp.sum((docs < d).astype(jnp.int32)) for d in (1, 2, 3)]
    heads = q_ref.shape[1] // HEAD_DIM
    lanes = heads * SPAN
    scale = math.log2(math.e) / math.sqrt(HEAD_DIM)
    within = lax.broadcasted_iota(jnp.int32, (1, lanes), 1) % SPAN

    queries, pos, low, first, count = [], [], [], [], []
    for half in range(2):
        rows = slice(half * SPAN, half * SPAN + SPAN)
        queries.append(
            jnp.concatenate(
                [q_ref[rows, h * HEAD_DIM : (h + 1) * HEAD_DIM] for h in range(heads)], axis=0
            )
        )
        at = spans[ctx * 2 + half] * SPAN
        pos.append(at + within)
        lo, lo0 = jnp.zeros_like(within), jnp.int32(0)
        for s in starts:
            lo = jnp.where(s <= pos[half], s, lo)
            lo0 = jnp.where(s <= at, s, lo0)
        low.append(lo)
        first.append(lo0 // CHUNK)
        count.append((at + SPAN - 1) // CHUNK - lo0 // CHUNK + 1)
    acc[...] = jnp.zeros_like(acc)
    kv_iota = lax.broadcasted_iota(jnp.int32, (CHUNK, lanes), 0)

    def step(t, carry):
        new = []
        for half in range(2):
            top, total = carry[half]
            chunk = first[half] + t
            safe = jnp.minimum(chunk, keys.shape[0] // CHUNK - 1)
            rows = pl.ds(pl.multiple_of(safe * CHUNK, CHUNK), CHUNK)
            scores = lax.dot_general(
                keys[rows, :], queries[half], (((1,), (1,)), ((), ())),
                preferred_element_type=jnp.float32,
            )
            kv_pos = kv_iota + chunk * CHUNK
            visible = (kv_pos >= low[half]) & (kv_pos <= pos[half])
            scores = jnp.where(visible, scores * scale, NEG)
            higher = jnp.maximum(top, jnp.max(scores, axis=0, keepdims=True))
            rescale = jnp.exp2(top - higher)
            probs = jnp.exp2(scores - higher)
            total = total * rescale + jnp.sum(probs, axis=0, keepdims=True)
            mixed = lax.dot_general(
                values[rows, :], probs.astype(jnp.bfloat16), (((0,), (0,)), ((), ())),
                preferred_element_type=jnp.float32,
            )
            acc[half] = acc[half] * rescale + mixed
            new.append((higher, total))
        return tuple(new)

    start = (jnp.full((1, lanes), NEG, jnp.float32), jnp.zeros((1, lanes), jnp.float32))
    done = lax.fori_loop(0, jnp.maximum(count[0], count[1]), step, (start, start))
    for half in range(2):
        mixed = acc[half] / done[half][1]
        for h in range(heads):
            part = mixed[:, h * SPAN : (h + 1) * SPAN].T
            out_ref[half * SPAN : half * SPAN + SPAN, h * HEAD_DIM : (h + 1) * HEAD_DIM] = (
                part.astype(jnp.bfloat16)
            )


ORDER = []


def attention(ctx, span_order, document, queries, blocks):
    ORDER[:] = [(dz, dc) for dz, dc, _ in blocks]
    seq = document.shape[0]
    rows, width = queries.shape
    return pl.pallas_call(
        attend_kernel,
        out_shape=jax.ShapeDtypeStruct((rows, width), jnp.bfloat16),
        in_specs=[SMEM, SMEM] + [VMEM] * (2 + len(blocks)),
        out_specs=VMEM,
        scratch_shapes=[
            pltpu.VMEM((seq, HEAD_DIM), jnp.bfloat16),
            pltpu.VMEM((seq, HEAD_DIM), jnp.bfloat16),
            pltpu.VMEM((2, HEAD_DIM, width), jnp.float32),
        ],
        compiler_params=pltpu.CompilerParams(vmem_limit_bytes=24 << 20),
        cost_estimate=pl.CostEstimate(
            flops=2 << 30, bytes_accessed=4 << 20, transcendentals=4 << 20
        ),
        name="attend",
    )(ctx, span_order, document.reshape(-1, SPAN), queries, *[b for _, _, b in blocks])


def project_kernel(where, att_ref, w_ref, *outs):
    rows = att_ref.shape[0] // 2
    cols = outs[0].shape[2]
    ex, why = where[1], where[2]
    att = att_ref[...]
    for kx in range(NX):
        for ky in range(NY):
            block = (ex + kx) % NX * NY + (why + ky) % NY
            at = pl.multiple_of(block * cols, cols)
            part = jnp.dot(att, w_ref[:, pl.ds(at, cols)], preferred_element_type=jnp.float32)
            part = part.astype(jnp.bfloat16)
            outs[kx][ky] = part[:rows]
            outs[NX + ky][kx] = part[rows:]


def projection(where, att, weight):
    rows = att.shape[0] // 2
    cols = weight.shape[1] // (NX * NY)
    return pl.pallas_call(
        project_kernel,
        out_shape=[jax.ShapeDtypeStruct((4, rows, cols), jnp.bfloat16)] * 8,
        in_specs=[SMEM, VMEM, VMEM],
        out_specs=[VMEM] * 8,
        compiler_params=pltpu.CompilerParams(vmem_limit_bytes=24 << 20),
        cost_estimate=pl.CostEstimate(
            flops=2 << 30, bytes_accessed=12 << 20, transcendentals=0
        ),
        name="project",
    )(where, att, weight)


def total_of(parts):
    return sum(p.astype(jnp.float32) for p in parts).astype(jnp.bfloat16)


def shards(queries, keys, values, out_weight, span_order, document):
    ctx, grp = lax.axis_index("ctx"), lax.axis_index("grp")
    where = jnp.stack([ctx, grp // NY, grp % NY]).astype(jnp.int32)
    local_heads = queries.shape[1] // HEAD_DIM
    at = grp * local_heads // QUERY_GROUP * HEAD_DIM
    own = jnp.concatenate(
        [lax.dynamic_slice_in_dim(a, at, HEAD_DIM, 1) for a in (keys, values)], axis=1
    )
    att = attention(where, span_order, document, queries, gathered(own))
    parts = projection(where, att, out_weight)
    by_x, by_y = parts[:4], parts[4:]
    got_x = [by_x[0]] + [lax.ppermute(by_x[k], "grp", along_x(k)) for k in (2, 1, 3)]
    got_y = [by_y[0]] + [lax.ppermute(by_y[k], "grp", along_y(k)) for k in (2, 1, 3)]
    next_y = [total_of([g[k] for g in got_x]) for k in range(4)]
    next_x = [total_of([g[k] for g in got_y]) for k in range(4)]
    last_x = [next_y[0]] + [lax.ppermute(next_y[k], "grp", along_y(k)) for k in (2, 1, 3)]
    last_y = [next_x[0]] + [lax.ppermute(next_x[k], "grp", along_x(k)) for k in (2, 1, 3)]
    return jnp.concatenate([total_of(last_x), total_of(last_y)], axis=0)


def solution(mesh):
    in_specs = (P("ctx", "grp"), P("ctx", None), P("ctx", None), P("grp", None), P(), P())
    out_specs = P("ctx", "grp")
    return jax.shard_map(shards, mesh=mesh, in_specs=in_specs, out_specs=out_specs, check_vma=False)
```

```python
import math

import jax
import jax.numpy as jnp
from jax import lax
from jax.experimental import pallas as pl
from jax.experimental.pallas import tpu as pltpu
from jax.sharding import PartitionSpec as P


HEAD_DIM = 128
QUERY_GROUP = 8
SPAN = 128
CHUNK = 256
NEG = -1e30
NZ, NX, NY = 8, 4, 4
FETCHES = 8

VMEM = pl.BlockSpec(memory_space=pltpu.VMEM)
SMEM = pl.BlockSpec(memory_space=pltpu.SMEM)
HBM = pl.BlockSpec(memory_space=pltpu.HBM)
BOTH = ("ctx", "grp")
STEPS = (2, 1, 3)

OTHER_CORE = [(i, i ^ 1) for i in range(2 * NZ)]
FAR_SIDE = [(z * 2 + c, (z + 4) % NZ * 2 + c) for z in range(NZ) for c in range(2)]


def ring(k):
    return [(z * 2 + c, (z + k * (1 - 2 * c)) % NZ * 2 + c) for z in range(NZ) for c in range(2)]


def plane_steps(k, x_core):
    pairs = []
    for ctx in range(2 * NZ):
        for x in range(NX):
            for y in range(NY):
                to = ((x + k) % NX, y) if ctx % 2 == x_core else (x, (y + k) % NY)
                pairs.append(((ctx * NX + x) * NY + y, (ctx * NX + to[0]) * NY + to[1]))
    return pairs


CAME = [(0, 0, 1), (0, 1, 1), (4, 0, 1), (4, 1, 1)]
CAME += [(-k, 0, 2) for k in (1, 2, 3)] + [(k, 1, 2) for k in (1, 2, 3)]


def gathered(own):
    other = lax.ppermute(own, "ctx", OTHER_CORE)
    chip = jnp.concatenate([own, other], axis=0)
    two = lax.ppermute(chip, "ctx", ring(2))
    one = lax.ppermute(chip, "ctx", ring(1))
    far = lax.ppermute(own, "ctx", FAR_SIDE)
    three = lax.ppermute(two, "ctx", ring(1))
    passed = [lax.ppermute(x, "ctx", OTHER_CORE) for x in (one, two, three)]
    return [own, other, far, lax.ppermute(far, "ctx", OTHER_CORE), one, two, three] + passed


def block_of(where, k, j):
    core, ex, why = where[0] % 2, where[1], where[2]
    by_x = (ex + k) % NX * NY + (why + j) % NY
    by_y = (ex + j) % NX * NY + (why + k) % NY
    return jnp.where(core == 0, by_x, by_y)


def project(where, att, w_ref, outs):
    cols = w_ref.shape[1] // (NX * NY)
    for k in STEPS + (0,):
        for j in range(4):
            at = pl.multiple_of(block_of(where, k, j) * cols, cols)
            part = jnp.dot(att, w_ref[:, pl.ds(at, cols)], preferred_element_type=jnp.float32)
            outs[k][j] = part.astype(jnp.bfloat16)


def fetch_kernel(where, w_hbm, w_ref, sems):
    rows = w_ref.shape[0] // FETCHES
    copies = [
        pltpu.make_async_copy(
            w_hbm.at[i * rows : (i + 1) * rows], w_ref.at[i * rows : (i + 1) * rows], sems.at[i]
        )
        for i in range(FETCHES)
    ]
    for copy in copies:
        copy.start()
    for copy in copies:
        copy.wait()


def fetched(where, weight):
    return pl.pallas_call(
        fetch_kernel,
        out_shape=jax.ShapeDtypeStruct(weight.shape, weight.dtype),
        in_specs=[SMEM, HBM],
        out_specs=VMEM,
        scratch_shapes=[pltpu.SemaphoreType.DMA((FETCHES,))],
        compiler_params=pltpu.CompilerParams(vmem_limit_bytes=40 << 20),
        cost_estimate=pl.CostEstimate(flops=0, bytes_accessed=16 << 20, transcendentals=0),
        name="fetch",
    )(where, weight)


def place(where, kv_refs, keys, values):
    zed, core = where[0] // 2, where[0] % 2
    for (steps, first, parts), kv in zip(CAME, kv_refs):
        plane = (zed + (steps if parts == 1 else steps * (1 - 2 * core)) + NZ) % NZ * 2
        for part in range(parts):
            source = plane + (core + first + part) % 2
            for half in range(2):
                at = pl.multiple_of(where[6 + source * 2 + half] * SPAN, SPAN)
                rows = slice((part * 2 + half) * SPAN, (part * 2 + half + 1) * SPAN)
                keys[pl.ds(at, SPAN), :] = kv[rows, :HEAD_DIM]
                values[pl.ds(at, SPAN), :] = kv[rows, HEAD_DIM:]


def attended(where, slot, q_ref, keys, values, acc):
    heads = q_ref.shape[1] // HEAD_DIM
    lanes = heads * SPAN
    scale = math.log2(math.e) / math.sqrt(HEAD_DIM)
    queries = jnp.concatenate(
        [q_ref[:, h * HEAD_DIM : (h + 1) * HEAD_DIM] for h in range(heads)], axis=0
    )
    at = where[6 + slot] * SPAN
    pos = at + lax.broadcasted_iota(jnp.int32, (1, lanes), 1) % SPAN
    low, low0 = jnp.zeros_like(pos), jnp.int32(0)
    for start in [where[i] for i in (3, 4, 5)]:
        low = jnp.where(start <= pos, start, low)
        low0 = jnp.where(start <= at, start, low0)
    acc[...] = jnp.zeros_like(acc)
    kv_iota = lax.broadcasted_iota(jnp.int32, (CHUNK, lanes), 0)

    def step(chunk, carry):
        top, total = carry
        rows = pl.ds(pl.multiple_of(chunk * CHUNK, CHUNK), CHUNK)
        scores = lax.dot_general(
            keys[rows, :], queries, (((1,), (1,)), ((), ())), preferred_element_type=jnp.float32
        )
        kv_pos = kv_iota + chunk * CHUNK
        visible = (kv_pos >= low) & (kv_pos <= pos)
        scores = jnp.where(visible, scores * scale, NEG)
        higher = jnp.maximum(top, jnp.max(scores, axis=0, keepdims=True))
        rescale = jnp.exp2(top - higher)
        probs = jnp.exp2(scores - higher)
        total = total * rescale + jnp.sum(probs, axis=0, keepdims=True)
        mixed = lax.dot_general(
            values[rows, :], probs.astype(jnp.bfloat16), (((0,), (0,)), ((), ())),
            preferred_element_type=jnp.float32,
        )
        acc[...] = acc[...] * rescale + mixed
        return higher, total

    start = (jnp.full((1, lanes), NEG, jnp.float32), jnp.zeros((1, lanes), jnp.float32))
    _, total = lax.fori_loop(low0 // CHUNK, (at + SPAN - 1) // CHUNK + 1, step, start)
    mixed = acc[...] / total
    return jnp.concatenate(
        [mixed[:, h * SPAN : (h + 1) * SPAN].T.astype(jnp.bfloat16) for h in range(heads)], axis=1
    )


def theirs_kernel(where, q_ref, w_ref, *refs):
    kv_refs, (keys, values), outs, acc = refs[:-7], refs[-7:-5], refs[-5:-1], refs[-1]
    place(where, kv_refs, keys, values)
    ctx = where[0]
    slot = (ctx // 2 * 2 + 1 - ctx % 2) * 2 + ctx % 2
    project(where, attended(where, slot, q_ref, keys, values, acc), w_ref, outs)


def mine_kernel(where, q_ref, w_ref, keys, values, *refs):
    outs, acc = refs[:4], refs[4]
    slot = where[0] * 2 + where[0] % 2
    project(where, attended(where, slot, q_ref, keys, values, acc), w_ref, outs)


def attend(kernel, where, queries, weight, kv, seq, keep):
    width = queries.shape[1]
    cols = weight.shape[1] // (NX * NY)
    kept = [jax.ShapeDtypeStruct((seq, HEAD_DIM), jnp.bfloat16)] * (2 * keep)
    parts = [jax.ShapeDtypeStruct((4, SPAN, cols), jnp.bfloat16)] * 4
    return pl.pallas_call(
        kernel,
        out_shape=kept + parts,
        in_specs=[SMEM] + [VMEM] * (2 + len(kv)),
        out_specs=[VMEM] * (len(kept) + 4),
        scratch_shapes=[pltpu.VMEM((HEAD_DIM, width), jnp.float32)],
        compiler_params=pltpu.CompilerParams(vmem_limit_bytes=24 << 20),
        cost_estimate=pl.CostEstimate(
            flops=2 << 30, bytes_accessed=12 << 20, transcendentals=2 << 20
        ),
    )(where, queries, weight, *kv)


def total_of(parts):
    return sum(p.astype(jnp.float32) for p in parts).astype(jnp.bfloat16)


def reduced(parts):
    got = [parts[0]]
    got += [lax.ppermute(parts[k], BOTH, plane_steps(k, 0)) for k in STEPS]
    line = [total_of([g[j] for g in got]) for j in range(4)]
    last = [lax.ppermute(line[j], BOTH, plane_steps(j, 1)) for j in STEPS]
    return total_of([line[0]] + last)


def shards(queries, keys, values, out_weight, span_order, document):
    ctx, grp = lax.axis_index("ctx"), lax.axis_index("grp")
    core = ctx % 2
    local_heads = queries.shape[1] // HEAD_DIM
    at = grp * local_heads // QUERY_GROUP * HEAD_DIM
    own = jnp.concatenate(
        [lax.dynamic_slice_in_dim(a, at, HEAD_DIM, 1) for a in (keys, values)], axis=1
    )
    kept = lax.dynamic_slice_in_dim(queries, core * SPAN, SPAN, 0)
    away = lax.dynamic_slice_in_dim(queries, (1 - core) * SPAN, SPAN, 0)
    swapped = lax.ppermute(away, "ctx", OTHER_CORE)
    starts = jnp.sum(document[None, :] < jnp.arange(1, 4)[:, None], axis=1, dtype=jnp.int32)
    index = jnp.stack([ctx, grp // NY, grp % NY]).astype(jnp.int32)
    where = jnp.concatenate([index, starts, span_order])
    weight = fetched(where, out_weight)
    blocks = gathered(own)
    seq = document.shape[0]
    *kv, b0, b1, b2, b3 = attend(theirs_kernel, where, swapped, weight, blocks, seq, True)
    parts = attend(mine_kernel, where, kept, weight, kv, seq, False)
    back = lax.ppermute(reduced([b0, b1, b2, b3]), "ctx", OTHER_CORE)
    mine = reduced(parts)
    return jnp.concatenate(
        [jnp.where(core == 0, mine, back), jnp.where(core == 0, back, mine)], axis=0
    )


def solution(mesh):
    in_specs = (P("ctx", "grp"), P("ctx", None), P("ctx", None), P("grp", None), P(), P())
    out_specs = P("ctx", "grp")
    return jax.shard_map(shards, mesh=mesh, in_specs=in_specs, out_specs=out_specs, check_vma=False)
```

```python
import math

import jax
import jax.numpy as jnp
from jax import lax
from jax.experimental import pallas as pl
from jax.experimental.pallas import tpu as pltpu
from jax.sharding import PartitionSpec as P


HEAD_DIM = 128
QUERY_GROUP = 8
SPAN = 128
CHUNK = 512
NEG = -1e30
NZ, NX, NY = 8, 4, 4
FETCHES = 8

VMEM = pl.BlockSpec(memory_space=pltpu.VMEM)
SMEM = pl.BlockSpec(memory_space=pltpu.SMEM)
HBM = pl.BlockSpec(memory_space=pltpu.HBM)
BOTH = ("ctx", "grp")
STEPS = (2, 1, 3, 0)
HALF = SPAN // 2

OTHER_CORE = [(i, i ^ 1) for i in range(2 * NZ)]


def ring(k):
    return [(z * 2 + c, (z + k * (1 - 2 * c)) % NZ * 2 + c) for z in range(NZ) for c in range(2)]


def plane_steps(k, x_core):
    pairs = []
    for ctx in range(2 * NZ):
        for x in range(NX):
            for y in range(NY):
                to = ((x + k) % NX, y) if ctx % 2 == x_core else (x, (y + k) % NY)
                pairs.append(((ctx * NX + x) * NY + y, (ctx * NX + to[0]) * NY + to[1]))
    return pairs


def sent(x, axis, pairs):
    return lax.ppermute(x, axis, pairs)


CAME = [(0, 0, 1), (0, 1, 1), (4, 0, 1), (4, 1, 1)]
CAME += [(-k, 0, 2) for k in (1, 2, 3)] + [(k, 1, 2) for k in (1, 2, 3)]


def gathered(own):
    other = sent(own, "ctx", OTHER_CORE)
    chip = jnp.concatenate([own, other], axis=0)
    two = sent(chip, "ctx", ring(2))
    one = sent(chip, "ctx", ring(1))
    three = sent(two, "ctx", ring(1))
    far = sent(two[: own.shape[0]], "ctx", ring(2))
    passed = [sent(x, "ctx", OTHER_CORE) for x in (one, two, three)]
    return [own, other, far, sent(far, "ctx", OTHER_CORE), one, two, three] + passed


def block_of(where, k, j):
    core, ex, why = where[0] % 2, where[1], where[2]
    by_x = (ex + k) % NX * NY + (why + j) % NY
    by_y = (ex + j) % NX * NY + (why + k) % NY
    return jnp.where(core == 0, by_x, by_y)


def project(where, att, w_ref, outs):
    up, down, up_add, down_add, kept = outs
    cols = w_ref.shape[1] // (NX * NY)
    top, low = slice(0, HALF), slice(HALF, SPAN)
    for k in STEPS:
        for j in range(4):
            at = pl.multiple_of(block_of(where, k, j) * cols, cols)
            part = jnp.dot(att, w_ref[:, pl.ds(at, cols)], preferred_element_type=jnp.float32)
            part = part.astype(jnp.bfloat16)
            if k == 2:
                up[0, j], down[0, j] = part[top], part[low]
            elif k == 1:
                up_add[j], up[1, j] = part[top], part[low]
            elif k == 3:
                down[1, j], down_add[j] = part[top], part[low]
            else:
                kept[j] = part


def parcels(cols):
    halves = jax.ShapeDtypeStruct((2, 4, HALF, cols), jnp.bfloat16)
    half = jax.ShapeDtypeStruct((4, HALF, cols), jnp.bfloat16)
    return [halves, halves, half, half, jax.ShapeDtypeStruct((4, SPAN, cols), jnp.bfloat16)]


def fetch_kernel(where, w_hbm, w_ref, sems):
    rows = w_ref.shape[0] // FETCHES
    copies = [
        pltpu.make_async_copy(
            w_hbm.at[i * rows : (i + 1) * rows], w_ref.at[i * rows : (i + 1) * rows], sems.at[i]
        )
        for i in range(FETCHES)
    ]
    for copy in copies:
        copy.start()
    for copy in copies:
        copy.wait()


def fetched(where, weight):
    return pl.pallas_call(
        fetch_kernel,
        out_shape=jax.ShapeDtypeStruct(weight.shape, weight.dtype),
        in_specs=[SMEM, HBM],
        out_specs=VMEM,
        scratch_shapes=[pltpu.SemaphoreType.DMA((FETCHES,))],
        compiler_params=pltpu.CompilerParams(vmem_limit_bytes=40 << 20),
        cost_estimate=pl.CostEstimate(flops=0, bytes_accessed=16 << 20, transcendentals=0),
        name="fetch",
    )(where, weight)


def place(where, kv_refs, keys, values):
    zed, core = where[0] // 2, where[0] % 2
    for (steps, first, parts), kv in zip(CAME, kv_refs):
        plane = (zed + (steps if parts == 1 else steps * (1 - 2 * core)) + NZ) % NZ * 2
        for part in range(parts):
            source = plane + (core + first + part) % 2
            for half in range(2):
                at = pl.multiple_of(where[6 + source * 2 + half] * SPAN, SPAN)
                rows = slice((part * 2 + half) * SPAN, (part * 2 + half + 1) * SPAN)
                keys[pl.ds(at, SPAN), :] = kv[rows, :HEAD_DIM]
                values[:, pl.ds(at, SPAN)] = kv[rows, HEAD_DIM:].T


def attended(where, slot, q_ref, keys, values, acc):
    heads = q_ref.shape[1] // HEAD_DIM
    lanes = heads * SPAN
    scale = math.log2(math.e) / math.sqrt(HEAD_DIM)
    queries = jnp.concatenate(
        [q_ref[:, h * HEAD_DIM : (h + 1) * HEAD_DIM].T for h in range(heads)], axis=1
    )
    at = where[6 + slot] * SPAN
    pos = at + lax.broadcasted_iota(jnp.int32, (1, lanes), 1) % SPAN
    low, low0 = jnp.zeros_like(pos), jnp.int32(0)
    for start in [where[i] for i in (3, 4, 5)]:
        low = jnp.where(start <= pos, start, low)
        low0 = jnp.where(start <= at, start, low0)
    acc[...] = jnp.zeros_like(acc)
    kv_iota = lax.broadcasted_iota(jnp.int32, (CHUNK, lanes), 0)

    def step(chunk, carry, masked):
        top, total = carry
        rows = pl.ds(pl.multiple_of(chunk * CHUNK, CHUNK), CHUNK)
        scores = lax.dot_general(
            keys[rows, :], queries, (((1,), (0,)), ((), ())), preferred_element_type=jnp.float32
        )
        scores = scores * scale
        if masked:
            kv_pos = kv_iota + chunk * CHUNK
            visible = (kv_pos >= low) & (kv_pos <= pos)
            scores = jnp.where(visible, scores, NEG)
        higher = jnp.maximum(top, jnp.max(scores, axis=0, keepdims=True))
        rescale = jnp.exp2(top - higher)
        probs = jnp.exp2(scores - higher)
        total = total * rescale + jnp.sum(probs, axis=0, keepdims=True)
        mixed = lax.dot_general(values[:, rows], probs.astype(jnp.bfloat16), (((1,), (0,)), ((), ())), preferred_element_type=jnp.float32)
        acc[...] = acc[...] * rescale + mixed
        return higher, total

    carry = (jnp.full((1, lanes), NEG, jnp.float32), jnp.zeros((1, lanes), jnp.float32))
    low1 = jnp.int32(0)
    for start in [where[i] for i in (3, 4, 5)]:
        low1 = jnp.where(start <= at + SPAN - 1, start, low1)
    begin, end = low0 // CHUNK, (at + SPAN - 1) // CHUNK + 1
    whole = jnp.clip((low1 + CHUNK - 1) // CHUNK, begin, end - 1)
    last = jnp.maximum(at // CHUNK, whole)
    carry = lax.fori_loop(begin, whole, lambda c, s: step(c, s, True), carry)
    carry = lax.fori_loop(whole, last, lambda c, s: step(c, s, False), carry)
    _, total = lax.fori_loop(last, end, lambda c, s: step(c, s, True), carry)
    mixed = acc[...] / total
    return jnp.concatenate(
        [mixed[:, h * SPAN : (h + 1) * SPAN].T.astype(jnp.bfloat16) for h in range(heads)], axis=1
    )


def theirs_kernel(where, q_ref, w_ref, *refs):
    kv_refs, (keys, values), outs, acc = refs[:-8], refs[-8:-6], refs[-6:-1], refs[-1]
    place(where, kv_refs, keys, values)
    ctx = where[0]
    slot = (ctx // 2 * 2 + 1 - ctx % 2) * 2 + ctx % 2
    project(where, attended(where, slot, q_ref, keys, values, acc), w_ref, outs)


def mine_kernel(where, q_ref, w_ref, keys, values, *refs):
    outs, acc = refs[:5], refs[5]
    slot = where[0] * 2 + where[0] % 2
    project(where, attended(where, slot, q_ref, keys, values, acc), w_ref, outs)


def attend(kernel, where, queries, weight, kv, seq, keep):
    width = queries.shape[1]
    cols = weight.shape[1] // (NX * NY)
    kept = [jax.ShapeDtypeStruct(d, jnp.bfloat16) for d in ((seq, HEAD_DIM), (HEAD_DIM, seq))] * keep
    parts = parcels(cols)
    return pl.pallas_call(
        kernel,
        out_shape=kept + parts,
        in_specs=[SMEM] + [VMEM] * (2 + len(kv)),
        out_specs=[VMEM] * (len(kept) + len(parts)),
        scratch_shapes=[pltpu.VMEM((HEAD_DIM, width), jnp.float32)],
        compiler_params=pltpu.CompilerParams(vmem_limit_bytes=24 << 20),
        cost_estimate=pl.CostEstimate(
            flops=2 << 30, bytes_accessed=12 << 20, transcendentals=2 << 20
        ),
    )(where, queries, weight, *kv)


def total_of(parts):
    return sum(p.astype(jnp.float32) for p in parts).astype(jnp.bfloat16)


def combine_kernel(kept, up, down, up_sum, down_sum, *outs):
    top, low = slice(0, HALF), slice(HALF, SPAN)
    for j, out in enumerate(outs):
        for rows, a, b in ((top, up_sum[j], down[1, j]), (low, up[1, j], down_sum[j])):
            out[rows] = (
                kept[j, rows].astype(jnp.float32) + a.astype(jnp.float32) + b.astype(jnp.float32)
            ).astype(jnp.bfloat16)


def combined(*parts):
    rows, cols = parts[0].shape[1:]
    return pl.pallas_call(
        combine_kernel,
        out_shape=[jax.ShapeDtypeStruct((rows, cols), jnp.bfloat16)] * 4,
        in_specs=[VMEM] * 5,
        out_specs=[VMEM] * 4,
        compiler_params=pltpu.CompilerParams(vmem_limit_bytes=16 << 20),
        cost_estimate=pl.CostEstimate(flops=1 << 20, bytes_accessed=2 << 20, transcendentals=0),
        name="combine",
    )(*parts)


def reduced(parts):
    up, down, up_add, down_add, kept = parts
    up = sent(up, BOTH, plane_steps(1, 0))
    down = sent(down, BOTH, plane_steps(3, 0))
    up_sum = sent(total_of([up_add, up[0]]), BOTH, plane_steps(1, 0))
    down_sum = sent(total_of([down_add, down[0]]), BOTH, plane_steps(3, 0))
    line = combined(kept, up, down, up_sum, down_sum)
    last = [sent(line[j], BOTH, plane_steps(j, 1)) for j in (2, 1, 3)]
    return [line[0]] + last


def finish_kernel(where, back, a, b, c, d, out_ref):
    core = where[0] % 2
    total = a[...].astype(jnp.float32) + b[...].astype(jnp.float32)
    total = total + c[...].astype(jnp.float32) + d[...].astype(jnp.float32)
    out_ref[pl.ds(pl.multiple_of(core * SPAN, SPAN), SPAN), :] = total.astype(jnp.bfloat16)
    out_ref[pl.ds(pl.multiple_of((1 - core) * SPAN, SPAN), SPAN), :] = back[...]


def finished(where, back, terms):
    return pl.pallas_call(
        finish_kernel,
        out_shape=jax.ShapeDtypeStruct((2 * SPAN, back.shape[1]), jnp.bfloat16),
        in_specs=[SMEM] + [VMEM] * 5,
        out_specs=VMEM,
        compiler_params=pltpu.CompilerParams(vmem_limit_bytes=16 << 20),
        cost_estimate=pl.CostEstimate(flops=1 << 18, bytes_accessed=1 << 20, transcendentals=0),
        name="finish",
    )(where, back, *terms)


def shards(queries, keys, values, out_weight, span_order, document):
    ctx, grp = lax.axis_index("ctx"), lax.axis_index("grp")
    core = ctx % 2
    local_heads = queries.shape[1] // HEAD_DIM
    at = grp * local_heads // QUERY_GROUP * HEAD_DIM
    own = jnp.concatenate(
        [lax.dynamic_slice_in_dim(a, at, HEAD_DIM, 1) for a in (keys, values)], axis=1
    )
    kept = lax.dynamic_slice_in_dim(queries, core * SPAN, SPAN, 0)
    away = lax.dynamic_slice_in_dim(queries, (1 - core) * SPAN, SPAN, 0)
    swapped = sent(away, "ctx", OTHER_CORE)
    starts = jnp.sum(document[None, :] < jnp.arange(1, 4)[:, None], axis=1, dtype=jnp.int32)
    index = jnp.stack([ctx, grp // NY, grp % NY]).astype(jnp.int32)
    where = jnp.concatenate([index, starts, span_order])
    weight = fetched(where, out_weight)
    blocks = gathered(own)
    seq = document.shape[0]
    *kv, up, down, up_add, down_add, own_part = attend(
        theirs_kernel, where, swapped, weight, blocks, seq, True
    )
    parts = attend(mine_kernel, where, kept, weight, kv, seq, False)
    back = sent(total_of(reduced([up, down, up_add, down_add, own_part])), "ctx", OTHER_CORE)
    return finished(where, back, reduced(parts))


def solution(mesh):
    in_specs = (P("ctx", "grp"), P("ctx", None), P("ctx", None), P("grp", None), P(), P())
    out_specs = P("ctx", "grp")
    return jax.shard_map(shards, mesh=mesh, in_specs=in_specs, out_specs=out_specs, check_vma=False)
```
